256 devices in a mesh: gx: 16 (over z_hi, y), gy: 16 (over z_lo, x, core).
Axes of the slice: x: 4, y: 4, z: 8 (z_hi: 4, z_lo: 2; z = z_hi * 2 + z_lo), core: 2. Of those that a mesh axis runs over, the one named last changes fastest.
Arguments:
- base_scores: float32 [12, 512, 256, 128], P(None, 'gx', 'gy'), may hold values from -6 to 6
- section_scores: float32 [12, 512, 256, 128], P(None, 'gx', 'gy'), may hold values from -6 to 6
- velocity: float32 [3, 512, 256, 128], P(None, 'gx', 'gy'), may hold values from -3 to 3
- diffusivity: float32 [512, 256, 128], P('gx', 'gy'), may hold values from 0.03 to 0.3
- w_first: bfloat16 [256, 12], replicated, may hold values from -1.75 to 1.75
- b_first: float32 [256], replicated, may hold values from -3 to 3
- w_second: bfloat16 [256, 256], replicated, may hold values from -0.375 to 0.375
- b_second: float32 [256], replicated, may hold values from -3 to 3
- w_third: bfloat16 [12, 256], replicated, may hold values from -0.375 to 0.375
- b_third: float32 [12], replicated, may hold values from -3 to 3
- loadings: bfloat16 [12, 300], replicated, may hold values from -0.375 to 0.375
- parcel_species: bfloat16 [8192, 300, 128], P(('gx', 'gy')), may hold values from -6 to 6
- parcel_owner: int32 [8192, 1], P(('gx', 'gy')), may hold values from 0 to 15; in each aligned block of 32 rows (0 to 31, 32 to 63, ...) at most 4 rows name the same one
- parcel_block: int32 [8192], P(('gx', 'gy')), may hold values from 0 to 31
Outputs:
- new_scores: float32 [12, 512, 256, 128], P(None, 'gx', 'gy')
The draws below stay inside these ranges and needn't reach their ends.
Inputs may be any that keep to these rules, and one draw needn't show every extreme that they name: `parcel_owner`: among the 32 parcel blocks of one device, no tile y index is named by more than 4 of them, and in every draw some device's blocks name one index exactly 4 times.
All inputs are finite; a program needn't handle non-finite values.
Results may differ from the reference program's by a relative error of at most 0.0003.
Values sent between devices are 32-bit elements; how exact they have to be, the bound alone decides.
A program may use at most 64 MiB of HBM per device.

```python
import math
import jax
import jax.numpy as jnp
import numpy as np
from jax import lax

NPC = 12
SPEC = 300
HID = 256
LX = 32
LY = 16
NZ = 128
CB = 128
SB = 32
PB = 32
CAP = 4
NX = 512
NY = 256
PBLK = 8192
N_GX = 16
N_GY = 16


def touch_ends(array, stream_key, least, high):
    spot = [jax.random.randint(jax.random.fold_in(stream_key, axis), (), 0, length) for axis, length in enumerate(array.shape)]
    main_axis = array.shape.index(max(array.shape))
    beside = spot[:main_axis] + [(spot[main_axis] + 1) % array.shape[main_axis]] + spot[main_axis + 1:]
    return array.at[tuple(spot)].set(least).at[tuple(beside)].set(high)


def shard_levels(rng, dims, cuts, low, high):
    def one(dim, blocks):
        draws = jax.random.uniform(jax.random.fold_in(jax.random.fold_in(rng, 6), dim), (blocks,), jnp.float32, low / len(cuts), high / len(cuts))
        return jnp.repeat(jnp.exp(draws), dims[dim] // blocks).reshape((-1,) + (1,) * (len(dims) - dim - 1))

    loudness = one(*cuts[0])
    for cut in cuts[1:]:
        loudness = loudness * one(*cut)
    return loudness


def routed_block(key, own, number, rows, amount, top, most, lean):
    order = jax.random.permutation(key, amount)
    crowded, common = load_shares(amount, rows * top, most, lean, True), load_shares(amount, rows * top, most, lean, False)
    places = jnp.arange(amount)

    def named(tallies, turn):
        used = int((tallies > 0).sum())
        fixed = max(1, used // 4)
        moved = fixed + (places - fixed + turn * (used - fixed)) % max(1, amount - fixed)
        return jnp.zeros((amount,), jnp.int32).at[order[jnp.where(places < fixed, places, moved)]].set(jnp.asarray(tallies, jnp.int32))

    tallies = jnp.where(number % 4 == 0, named(crowded, number // 4), named(common, number - number // 4 - 1))
    mixed = jax.random.permutation(jax.random.fold_in(own, 3), amount)
    giver, sink = mixed[0:amount // 2 * 2:2], mixed[1:amount // 2 * 2:2]
    slack = jnp.minimum(tallies[giver] - 1, most - tallies[sink]) // 2
    slack = jnp.where((giver == order[0]) | (sink == order[0]) | (tallies[sink] == 0), 0, jnp.maximum(slack, 0))
    moved = jax.random.randint(jax.random.fold_in(own, 4), (amount // 2,), 0, 1 << 20) % (slack + 1)
    tallies = tallies.at[giver].add(-moved).at[sink].add(moved)
    labels = jnp.searchsorted(jnp.cumsum(tallies), jnp.arange(rows * top), side="right").astype(jnp.int32)
    table = labels.reshape(top, rows).T
    table = table[jax.random.permutation(jax.random.fold_in(own, 1), rows)]
    turn = jax.random.randint(jax.random.fold_in(own, 2), (rows, 1), 0, top)
    return jnp.take_along_axis(table, (jnp.arange(top)[None, :] + turn) % top, axis=1)


def load_shares(amount, total, most, lean, full):
    loads = [(1 << 20) // math.isqrt(standing ** lean) + 1 for standing in range(1, amount + 1)]
    largest = most if full else min(most, max(-(-total // amount), total * loads[0] // sum(loads)))
    least = 1 if total - largest >= amount - 1 else 0
    holding, rest = [largest] + [least] * (amount - 1), total - largest - least * (amount - 1)
    while rest > 0:
        movable = [i for i in range(1, amount) if holding[i] < largest] or [i for i in range(1, amount) if holding[i] < most]
        whole, budget = sum([loads[i] for i in movable]), rest
        for i in movable:
            more = min(most - holding[i], max(1, budget * loads[i] // whole), rest)
            holding[i] = holding[i] + more
            rest = rest - more
    return np.array(holding)


def normal_values(key, shape, scale, most, cuts=(), kind=jnp.bfloat16):
    values = scale * jax.random.normal(key, shape, jnp.float32)
    if cuts:
        values = values * shard_levels(key, shape, cuts, -0.22, 0.18)
    return jnp.clip(values, -most, most).astype(kind)


def setup_inputs(seed: int = 0) -> dict:
    keys = jax.random.split(jax.random.key(seed), 15)
    base_scores = normal_values(keys[0], (NPC, NX, NY, NZ), 1.0, 6.0, ((1, 16), (2, 16)), jnp.float32)
    section_scores = normal_values(keys[1], (NPC, NX, NY, NZ), 1.0, 6.0, ((1, 16), (2, 16)), jnp.float32)
    velocity = normal_values(keys[2], (3, NX, NY, NZ), 0.6, 3.0, ((1, 16), (2, 16)), jnp.float32)
    diffusivity = jnp.clip(jnp.exp(math.log(0.3) - 2.3025852 * jax.random.uniform(keys[3], (NX, NY, NZ), jnp.float32) ** shard_levels(keys[3], (NX, NY, NZ), ((0, 16), (1, 16)), -0.2, 0.2)), 0.03, 0.3)
    w_first = normal_values(keys[4], (HID, NPC), NPC ** -0.5, 1.75)
    b_first = normal_values(keys[5], (HID,), 0.5, 3.0, (), jnp.float32)
    w_second = normal_values(keys[6], (HID, HID), HID ** -0.5, 0.375)
    b_second = normal_values(keys[7], (HID,), 0.5, 3.0, (), jnp.float32)
    w_third = normal_values(keys[8], (NPC, HID), HID ** -0.5, 0.375)
    b_third = normal_values(keys[9], (NPC,), 0.5, 3.0, (), jnp.float32)
    loadings = normal_values(keys[10], (NPC, SPEC), SPEC ** -0.5, 0.375)
    parcel_species = normal_values(keys[11], (PBLK, SPEC, CB), 1.0, 6.0, ((0, 256),))
    parcel_owner_keys = jax.random.split(jax.random.fold_in(keys[12], 1), PBLK // PB)
    parcel_owner_turns = jax.random.permutation(jax.random.fold_in(keys[12], 3), PBLK // PB)
    parcel_owner = jax.vmap(lambda own, number: routed_block(jax.random.fold_in(keys[12], 2), own, number, PB, N_GY, 1, CAP, 2))(parcel_owner_keys, parcel_owner_turns).reshape((PBLK, 1))
    parcel_block = touch_ends(jax.random.randint(keys[13], (PBLK,), 0, SB), jax.random.fold_in(keys[13], 1), 0, SB - 1).astype(jnp.int32)
    return dict(base_scores=base_scores, section_scores=section_scores, velocity=velocity, diffusivity=diffusivity, w_first=w_first, b_first=b_first, w_second=w_second, b_second=b_second, w_third=w_third, b_third=b_third, loadings=loadings, parcel_species=parcel_species, parcel_owner=parcel_owner, parcel_block=parcel_block)


dt_step = 0.25


def regress(block, w_first, b_first, w_second, b_second, w_third, b_third):
    inputs = block.astype(jnp.bfloat16)
    first = jnp.tanh(jnp.dot(w_first, inputs, preferred_element_type=jnp.float32) + b_first[:, None]).astype(jnp.bfloat16)
    second = jnp.tanh(jnp.dot(w_second, first, preferred_element_type=jnp.float32) + b_second[:, None]).astype(jnp.bfloat16)
    return jnp.dot(w_third, second, preferred_element_type=jnp.float32) + b_third[:, None]


def sources(flat, weights):
    comps, count = flat.shape
    width = math.gcd(count, 4096)
    blocks = flat.reshape(comps, count // width, width).transpose(1, 0, 2)
    result = lax.map(lambda piece: regress(piece, *weights), blocks)
    return result.transpose(1, 0, 2).reshape(comps, count)


def transport_rate(center, plus_x, minus_x, plus_y, minus_y, plus_z, minus_z, velocity, diffusivity):
    drift = velocity[0] * (plus_x - minus_x) + velocity[1] * (plus_y - minus_y) + velocity[2] * (plus_z - minus_z)
    spread = plus_x + minus_x + plus_y + minus_y + plus_z + minus_z - 6.0 * center
    return diffusivity * spread - 0.5 * drift


def reference(base_scores, section_scores, velocity, diffusivity, w_first, b_first, w_second, b_second, w_third, b_third, loadings, parcel_species, parcel_owner, parcel_block):
    def one_score(field):
        padded = jnp.pad(field, 1)
        return transport_rate(field, padded[2:, 1:-1, 1:-1], padded[:-2, 1:-1, 1:-1], padded[1:-1, 2:, 1:-1], padded[1:-1, :-2, 1:-1], padded[1:-1, 1:-1, 2:], padded[1:-1, 1:-1, :-2], velocity, diffusivity)

    transport = lax.map(one_score, section_scores)
    weights = (w_first, b_first, w_second, b_second, w_third, b_third)
    chemistry = sources(section_scores.reshape(NPC, -1), weights).reshape(section_scores.shape)
    total = PB * N_GX * N_GY
    grouped = parcel_species.reshape(total // PB, PB, SPEC, CB)
    load_wide = loadings.astype(jnp.float32)
    projected = lax.map(lambda group: jnp.einsum("ks,psc->pkc", load_wide, group.astype(jnp.float32), precision=lax.Precision.HIGHEST).astype(jnp.bfloat16), grouped)
    projected = lax.optimization_barrier(projected)
    projected = projected.reshape(total, NPC * CB).astype(jnp.float32)
    source_row = (jnp.arange(total, dtype=jnp.int32) // (PB * N_GY)).astype(jnp.int32)
    segment = ((source_row * N_GY + parcel_owner[:, 0]) * SB + parcel_block).astype(jnp.int32)
    deposit = jax.ops.segment_sum(projected, segment, num_segments=N_GX * N_GY * SB)
    deposit = deposit.reshape(N_GX, N_GY, SB, NPC, CB).transpose(3, 0, 1, 2, 4).reshape(NPC, N_GX, N_GY, SB * CB)
    cells = LX * LY * NZ
    deposit = jnp.pad(deposit, ((0, 0), (0, 0), (0, 0), (0, cells - SB * CB)))
    spray = deposit.reshape(NPC, N_GX, N_GY, LX, LY, NZ).transpose(0, 1, 3, 2, 4, 5).reshape(NPC, N_GX * LX, N_GY * LY, NZ)
    rate = transport + chemistry + spray
    return 0.75 * base_scores + 0.25 * (section_scores + dt_step * rate)
```

```python
import jax
import jax.numpy as jnp
from jax import lax
from jax.experimental import pallas as pl
from jax.experimental.pallas import tpu as pltpu
from jax.sharding import PartitionSpec as P

BF = jnp.bfloat16
F32 = jnp.float32
MESH = pl.DeviceIdType.MESH

NPC = 12
SPEC = 300
SPAD = 304
HID = 256
LX, LY, NZ = 32, 16, 128
PB = 32
CAP = 4
SB = 32
NG = 16
CH = 8
NCH = LX // CH
PAIRS = CH // 2
LAG = 2
DT = 0.25
WIDE = (NPC + 1) * NZ
CROWS = 144


def iota(shape, dim):
    return lax.broadcasted_iota(jnp.int32, shape, dim)


def kernel(
    base, section, edges, velocity, diffusivity, w1t, b1, w2, b2, w3, b3, loadings, parcels, owner, block,
    result,
    sec, basev, velv, diffv, outv, chem, par, weave, lrep, lpad, ylo, yhi, send, recv, spr,
    w1tv, b1v, w2v, b2v, w3v, ownv, blkv, loadv, b3s, a16, w1s, b2c, w3p, b3c,
    in_sem, chunk_sem, out_sem, xs, xr, ys, yr, ssem, rsem,
):
    gx = lax.axis_index("gx")
    gy = lax.axis_index("gy")

    barrier = pltpu.get_barrier_semaphore()
    for d in range(1, NG):
        pl.semaphore_signal(barrier, inc=1, device_id={"gy": lax.rem(gy + d, NG)}, device_id_type=MESH)

    @pl.when(gx > 0)
    def _():
        pl.semaphore_signal(barrier, inc=1, device_id={"gx": gx - 1}, device_id_type=MESH)

    @pl.when(gx < NG - 1)
    def _():
        pl.semaphore_signal(barrier, inc=1, device_id={"gx": gx + 1}, device_id_type=MESH)

    small = [
        pltpu.make_async_copy(a, b, in_sem.at[i])
        for i, (a, b) in enumerate(
            [(w1t, w1tv), (b1, b1v), (w2, w2v), (b2, b2v), (w3, w3v), (b3, b3s), (loadings, loadv), (owner, ownv), (block, blkv)]
        )
    ]
    for c in small:
        c.start()

    def chunk_copy(c):
        return pltpu.make_async_copy(
            section.at[:, pl.ds(CH * c, CH)], sec.at[:, pl.ds(1 + CH * c, CH), pl.ds(8, LY)], chunk_sem.at[c]
        )

    for c in (1, 2, 3, 0):
        chunk_copy(c).start()
    big = [
        pltpu.make_async_copy(a, b, in_sem.at[9 + i])
        for i, (a, b) in enumerate([(parcels, par.at[pl.ds(0, SPEC)]), (velocity, velv), (diffusivity, diffv), (base, basev)])
    ]
    for c in big:
        c.start()

    for c in small:
        c.wait()
    par[SPEC:SPAD] = jnp.zeros((SPAD - SPEC, PB, NZ), BF)
    bias = b1v[...]
    hi = bias.astype(BF).astype(F32)
    mid = (bias - hi).astype(BF).astype(F32)
    a16[0:NPC, :] = w1tv[...].astype(F32)
    a16[12:13, :] = hi
    a16[13:14, :] = mid
    a16[14:15, :] = (bias - hi) - mid
    a16[15:16, :] = jnp.zeros((1, HID), F32)
    left = a16[...].T.astype(BF)
    row, lane = iota((16, NZ), 0), iota((16, NZ), 1)
    for j in range(8):
        pick = ((lane < 96) & (lane // 8 == row) & (lane % 8 == j)) | ((lane >= 96) & (lane - 96 + 12 == row) & (row < 15))
        w1s[j] = jnp.dot(left, pick.astype(F32).astype(BF), preferred_element_type=F32).astype(BF)
    b2c[...] = jnp.broadcast_to(b2v[...], (NZ, HID)).T
    w3p[...] = jnp.zeros((16, HID), BF)
    w3p[0:NPC, :] = (w3v[...].astype(F32) * (0.25 * DT)).astype(BF)
    col = jnp.zeros((16, NZ), F32)
    for k in range(NPC):
        col = jnp.where(row == k, b3s[0, k] * (0.25 * DT), col)
    b3c[...] = col
    lpad[...] = jnp.zeros((16, 384), F32)
    lpad[0:NPC, 0:SPEC] = loadv[...].astype(F32)
    for g in range(SPAD // 8):
        tile = lpad[:, (8 * g // 128) * 128 : (8 * g // 128) * 128 + 128]
        lrep[:, 128 * g : 128 * g + 128] = jnp.take_along_axis(tile, (8 * g) % 128 + lane // 16, axis=1)
    diagonal = (iota((16, 256), 1) % 16) == iota((16, 256), 0)

    def weave_one(c, carry):
        for k in range(NPC):
            line = lrep[k : k + 1, pl.ds(pl.multiple_of(256 * c, 256), 256)]
            weave[c, 16 * k : 16 * k + 16, :] = jnp.where(diagonal, jnp.broadcast_to(line, (16, 256)), 0.0).astype(BF)
        return carry

    lax.fori_loop(0, SPAD // 16, weave_one, 0)

    pl.semaphore_wait(barrier, NG - 1 + (gx > 0).astype(jnp.int32) + (gx < NG - 1).astype(jnp.int32))

    def halo_x(up):
        return pltpu.make_async_remote_copy(
            section.at[:, LX - 1 if up else 0], sec.at[:, 0 if up else LX + 1, pl.ds(8, LY)],
            xs.at[0 if up else 1], xr.at[0 if up else 1],
            device_id={"gx": gx + 1 if up else gx - 1}, device_id_type=MESH,
        )

    def halo_y(up):
        return pltpu.make_async_remote_copy(
            edges.at[:, :, LY - 1 if up else 0], ylo if up else yhi,
            ys.at[0 if up else 1], yr.at[0 if up else 1],
            device_id={"gy": gy + 1 if up else gy - 1}, device_id_type=MESH,
        )

    pl.when(gy < NG - 1)(lambda: halo_y(True).start())
    pl.when(gy > 0)(lambda: halo_y(False).start())
    pl.when(gx < NG - 1)(lambda: halo_x(True).start())
    pl.when(gx > 0)(lambda: halo_x(False).start())

    def regress(c, aside):
        n = 8 * PAIRS
        ones = (iota((32, NZ), 0) < 3).astype(F32).astype(BF)
        bias2 = jnp.concatenate([b2c[...]] * 4, axis=1)
        bias3 = jnp.concatenate([b3c[...]] * 4, axis=1)
        cells, first, second = {}, {}, {}
        for t in range(n + 2 * LAG):
            if t < n:
                if t % 8 == 0:
                    parts = []
                    for dx in range(2):
                        for o in range(2):
                            v = sec[:, CH * c + 1 + 2 * (t // 8) + dx, 8 + 8 * o : 16 + 8 * o, :]
                            parts.append(jnp.concatenate([v.reshape(96, NZ).astype(BF), ones], axis=0))
                    cells[t // 8] = jnp.concatenate(parts, axis=1)
                one = jnp.dot(w1s[t % 8], cells[t // 8], preferred_element_type=F32)
            if LAG <= t < n + LAG:
                two = jnp.dot(w2v[...], first.pop(t - LAG), preferred_element_type=F32)
            if t >= 2 * LAG:
                u = t - 2 * LAG
                three = jnp.dot(w3p[...], second.pop(u), preferred_element_type=F32) + bias3
                for dx in range(2):
                    for o in range(2):
                        h = 2 * dx + o
                        chem[CH * c + 2 * (u // 8) + dx, o, pl.ds(u % 8, 16, stride=9), :] = three[:, NZ * h : NZ * h + NZ]
            if t < n:
                first[t] = jnp.tanh(one).astype(BF)
            if LAG <= t < n + LAG:
                second[t - LAG] = jnp.tanh(two + bias2).astype(BF)
            aside(t)

    lane3 = iota((LY, NZ), 1)

    def combine(x, extra=None):
        e = x + 1
        sec[:, e, 7:8, :] = ylo[:, x]
        sec[:, e, 24:25, :] = yhi[:, x]
        d = diffv[x] * (0.25 * DT)
        vx, vy, vz = (velv[i, x] * (-0.125 * DT) for i in range(3))
        up = jnp.where(lane3 == NZ - 1, 0.0, d + vz)
        down = jnp.where(lane3 == 0, 0.0, d - vz)
        c = sec[:, e, 8:24, :]
        total = 0.75 * basev[:, x] + (0.25 - 6.0 * d) * c
        total += (d + vx) * sec[:, e + 1, 8:24, :] + (d - vx) * sec[:, e - 1, 8:24, :]
        total += (d + vy) * sec[:, e, 9:25, :] + (d - vy) * sec[:, e, 7:23, :]
        total += up * pltpu.roll(c, NZ - 1, axis=2) + down * pltpu.roll(c, 1, axis=2)
        if extra is not None:
            total += spr[extra]
        for k in range(NPC):
            for o in range(2):
                outv[k, x, 8 * o : 8 * o + 8, :] = total[k, 8 * o : 8 * o + 8] + chem[x, o, 9 * k : 9 * k + 8, :]

    def out_copy(c):
        return pltpu.make_async_copy(outv.at[:, pl.ds(CH * c, CH)], result.at[:, pl.ds(CH * c, CH)], out_sem.at[c])

    chunk_copy(1).wait()
    regress(1, lambda t: None)

    big[0].wait()
    projected = jnp.zeros((NPC * 16, 2 * NZ), F32)
    for c in range(SPAD // 16):
        right = jnp.concatenate(
            [par[16 * c : 16 * c + 16, 16 * h : 16 * h + 16, :].reshape(256, NZ) for h in range(2)], axis=1
        )
        projected += jnp.dot(weave[c], right, preferred_element_type=F32)
    projected = projected.astype(BF)
    eye = iota((PB, PB), 0) == iota((PB, PB), 1)
    own_row = jnp.broadcast_to(ownv[...].astype(F32), (PB, PB))
    own_col = jnp.sum(jnp.where(eye, own_row, 0.0), axis=1, keepdims=True)
    earlier = (own_row == own_col) & (iota((PB, PB), 0) < iota((PB, PB), 1))
    rank = jnp.sum(jnp.where(earlier, 1.0, 0.0), axis=0, keepdims=True)
    slot = jnp.broadcast_to(ownv[...].astype(F32) * CAP + rank, (NG * CAP, PB))
    chosen = (slot == iota((NG * CAP, PB), 0).astype(F32)).astype(F32).astype(BF)
    blk_row = jnp.broadcast_to(blkv[...].astype(F32) + 1.0, (PB, PB))
    tag = jnp.broadcast_to(jnp.sum(jnp.where(eye, blk_row, 0.0), axis=1, keepdims=True), (PB, NZ)).astype(BF)
    pieces = [
        jnp.concatenate([projected[16 * k : 16 * k + 16, 0:NZ], projected[16 * k : 16 * k + 16, NZ : 2 * NZ]], axis=0)
        for k in range(NPC)
    ]
    values = jnp.dot(chosen, jnp.concatenate(pieces + [tag], axis=1), preferred_element_type=F32)
    for i in range(NG):
        send[i] = values[CAP * i : CAP * i + CAP, :]
    recv[gy] = send[gy]

    def exchange(d):
        peer = lax.rem(gy + d, NG)
        return pltpu.make_async_remote_copy(
            send.at[peer], recv.at[gy], ssem.at[d], rsem.at[d], device_id={"gy": peer}, device_id_type=MESH
        )

    for d in range(1, NG):
        exchange(d).start()

    @pl.when(gx > 0)
    def _():
        halo_x(True).wait_recv()

    @pl.when(gx == 0)
    def _():
        sec[:, 0, 8:24, :] = jnp.zeros((NPC, LY, NZ), F32)

    @pl.when(gx < NG - 1)
    def _():
        halo_x(False).wait_recv()

    @pl.when(gx == NG - 1)
    def _():
        sec[:, LX + 1, 8:24, :] = jnp.zeros((NPC, LY, NZ), F32)

    @pl.when(gy > 0)
    def _():
        halo_y(True).wait_recv()

    @pl.when(gy == 0)
    def _():
        ylo[...] = jnp.zeros((NPC, LX, 1, NZ), F32)

    @pl.when(gy < NG - 1)
    def _():
        halo_y(False).wait_recv()

    @pl.when(gy == NG - 1)
    def _():
        yhi[...] = jnp.zeros((NPC, LX, 1, NZ), F32)

    for c in (2, 3, 0):
        chunk_copy(c).wait()
    for c in big[1:]:
        c.wait()

    def step(b, carry):
        @pl.when(b == NCH - 1)
        def _():
            for d in range(1, NG):
                exchange(d).wait_recv()
            got = jnp.concatenate([recv[i] for i in range(NG)], axis=0)
            place = (got[:, NPC * NZ :] - 1.0 == iota((NG * CAP, NZ), 1).astype(F32)).astype(F32).T[0:SB].astype(BF)
            mine = jnp.dot(place, got[:, 0 : NPC * NZ].astype(BF), preferred_element_type=F32) * (0.25 * DT)
            for k in range(NPC):
                for x in range(2):
                    spr[x, k] = mine[LY * x : LY * x + LY, NZ * k : NZ * k + NZ]

        def aside(t):
            if t % 4 == 2 and t // 4 < CH:
                combine(CH * b + t // 4)

        regress(lax.rem(b + 1, NCH), aside)
        out_copy(b).start()
        return carry

    lax.fori_loop(1, NCH, step, 0)
    for x in range(CH):
        combine(x, x if x < 2 else None)
    out_copy(0).start()
    for d in range(1, NG):
        exchange(d).wait_send()
    pl.when(gy < NG - 1)(lambda: halo_y(True).wait_send())
    pl.when(gy > 0)(lambda: halo_y(False).wait_send())
    pl.when(gx < NG - 1)(lambda: halo_x(True).wait_send())
    pl.when(gx > 0)(lambda: halo_x(False).wait_send())
    for c in range(NCH):
        out_copy(c).wait()


def shards(
    base_scores, section_scores, velocity, diffusivity, w_first, b_first, w_second, b_second, w_third, b_third,
    loadings, parcel_species, parcel_owner, parcel_block,
):
    anywhere = pl.BlockSpec(memory_space=pl.ANY)
    vmem = pltpu.VMEM
    dma = pltpu.SemaphoreType.DMA
    return pl.pallas_call(
        kernel,
        out_shape=jax.ShapeDtypeStruct((NPC, LX, LY, NZ), F32),
        in_specs=[anywhere] * 15,
        out_specs=anywhere,
        scratch_shapes=[
            vmem((NPC, LX + 2, 2 * LY, NZ), F32),
            vmem((NPC, LX, LY, NZ), F32),
            vmem((3, LX, LY, NZ), F32),
            vmem((LX, LY, NZ), F32),
            vmem((NPC, LX, LY, NZ), F32),
            vmem((LX, 2, CROWS, NZ), F32),
            vmem((SPAD, PB, NZ), BF),
            vmem((SPAD // 16, NPC * 16, 256), BF),
            vmem((16, SPAD * 16), F32),
            vmem((16, 384), F32),
            vmem((NPC, LX, 1, NZ), F32),
            vmem((NPC, LX, 1, NZ), F32),
            vmem((NG, CAP, WIDE), F32),
            vmem((NG, CAP, WIDE), F32),
            vmem((2, NPC, LY, NZ), F32),
            vmem((NPC, HID), BF),
            vmem((1, HID), F32),
            vmem((HID, HID), BF),
            vmem((1, HID), F32),
            vmem((NPC, HID), BF),
            vmem((1, PB), jnp.int32),
            vmem((1, PB), jnp.int32),
            vmem((NPC, SPEC), BF),
            pltpu.SMEM((1, NPC), F32),
            vmem((16, HID), F32),
            vmem((8, HID, NZ), BF),
            vmem((HID, NZ), F32),
            vmem((16, HID), BF),
            vmem((16, NZ), F32),
            dma((13,)),
            dma((NCH,)),
            dma((NCH,)),
            dma((2,)),
            dma((2,)),
            dma((2,)),
            dma((2,)),
            dma((NG,)),
            dma((NG,)),
        ],
        compiler_params=pltpu.CompilerParams(collective_id=0, has_side_effects=True),
        name="section_step",
    )(
        base_scores, section_scores, section_scores.reshape(NPC, LX, LY, 1, NZ), velocity, diffusivity,
        w_first.T, b_first.reshape(1, HID), w_second, b_second.reshape(1, HID), w_third, b_third.reshape(1, NPC),
        loadings, parcel_species.transpose(1, 0, 2), parcel_owner.reshape(1, PB), parcel_block.reshape(1, PB),
    )


def solution(mesh):
    placed = (
        P(None, "gx", "gy", None), P(None, "gx", "gy", None), P(None, "gx", "gy", None), P("gx", "gy", None),
        P(), P(), P(), P(), P(), P(), P(),
        P(("gx", "gy"), None, None), P(("gx", "gy"), None), P(("gx", "gy")),
    )
    return jax.shard_map(
        shards, mesh=mesh, in_specs=placed, out_specs=P(None, "gx", "gy", None), check_vma=False
    )
```

```python
import jax
import jax.numpy as jnp
from jax import lax
from jax.experimental import pallas as pl
from jax.experimental.pallas import tpu as pltpu
from jax.sharding import PartitionSpec as P

BF = jnp.bfloat16
F32 = jnp.float32
MESH = pl.DeviceIdType.MESH

NPC = 12
SPEC = 300
SPAD = 320
PART = 60
HID = 256
LX, LY, NZ = 32, 16, 128
PB = 32
CAP = 4
SB = 32
NG = 16
CH = 4
NCH = LX // CH
PAIRS = CH // 2
LAG = 2
DT = 0.25
WIDE = (NPC + 1) * NZ
CROWS = 144


def iota(shape, dim):
    return lax.broadcasted_iota(jnp.int32, shape, dim)


def kernel(
    base, section, edges, velocity, diffusivity, w1t, b1, w2, b2, w3, b3, loadings, parcels, owner, block,
    result,
    sec, basev, velv, diffv, chem, par, proj, lrep, lpad, ylo, yhi, send, recv, spr,
    w1tv, b1v, w2v, b2v, w3v, ownv, blkv, loadv, b3s, a16, w1s, b2c, w3p, b3c,
    in_sem, par_sem, chunk_sem, xs, xr, ys, yr, ssem, rsem,
):
    gx = lax.axis_index("gx")
    gy = lax.axis_index("gy")

    barrier = pltpu.get_barrier_semaphore()
    for d in range(1, NG):
        pl.semaphore_signal(barrier, inc=1, device_id={"gy": lax.rem(gy + d, NG)}, device_id_type=MESH)

    @pl.when(gx > 0)
    def _():
        pl.semaphore_signal(barrier, inc=1, device_id={"gx": gx - 1}, device_id_type=MESH)

    @pl.when(gx < NG - 1)
    def _():
        pl.semaphore_signal(barrier, inc=1, device_id={"gx": gx + 1}, device_id_type=MESH)

    small = [
        pltpu.make_async_copy(a, b, in_sem.at[i])
        for i, (a, b) in enumerate(
            [(w1t, w1tv), (b1, b1v), (w2, w2v), (b2, b2v), (w3, w3v), (b3, b3s), (loadings, loadv), (owner, ownv), (block, blkv)]
        )
    ]
    for c in small:
        c.start()

    def chunk_copy(c):
        return pltpu.make_async_copy(
            section.at[:, pl.ds(CH * c, CH)], sec.at[:, pl.ds(1 + CH * c, CH), pl.ds(8, LY)], chunk_sem.at[c]
        )

    def parcel_copy(i):
        return pltpu.make_async_copy(parcels.at[pl.ds(PART * i, PART)], par.at[pl.ds(PART * i, PART)], par_sem.at[i])

    chunk_copy(1).start()
    parcel_copy(0).start()
    parcel_copy(1).start()
    chunk_copy(2).start()
    parcel_copy(2).start()
    chunk_copy(3).start()
    parcel_copy(3).start()
    chunk_copy(4).start()
    parcel_copy(4).start()
    for c in (5, 6, 7, 0):
        chunk_copy(c).start()
    big = [
        pltpu.make_async_copy(a, b, in_sem.at[9 + i])
        for i, (a, b) in enumerate([(velocity, velv), (diffusivity, diffv), (base, basev)])
    ]
    for c in big:
        c.start()

    for c in small:
        c.wait()
    par[SPEC:SPAD] = jnp.zeros((SPAD - SPEC, PB, NZ), BF)
    bias = b1v[...]
    hi = bias.astype(BF).astype(F32)
    mid = (bias - hi).astype(BF).astype(F32)
    a16[0:NPC, :] = w1tv[...].astype(F32)
    a16[12:13, :] = hi
    a16[13:14, :] = mid
    a16[14:15, :] = (bias - hi) - mid
    a16[15:16, :] = jnp.zeros((1, HID), F32)
    left = a16[...].T.astype(BF)
    row, lane = iota((16, NZ), 0), iota((16, NZ), 1)
    for j in range(8):
        pick = ((lane < 96) & (lane // 8 == row) & (lane % 8 == j)) | ((lane >= 96) & (lane - 96 + 12 == row) & (row < 15))
        w1s[j] = jnp.dot(left, pick.astype(F32).astype(BF), preferred_element_type=F32).astype(BF)
    b2c[...] = jnp.broadcast_to(b2v[...], (NZ, HID)).T
    w3p[...] = jnp.zeros((16, HID), BF)
    w3p[0:NPC, :] = (w3v[...].astype(F32) * (0.25 * DT)).astype(BF)
    col = jnp.zeros((16, NZ), F32)
    for k in range(NPC):
        col = jnp.where(row == k, b3s[0, k] * (0.25 * DT), col)
    b3c[...] = col
    lpad[...] = jnp.zeros((16, 384), F32)
    lpad[0:NPC, 0:SPEC] = loadv[...].astype(F32)
    for g in range(SPAD // 8):
        tile = lpad[:, (8 * g // 128) * 128 : (8 * g // 128) * 128 + 128]
        lrep[:, 128 * g : 128 * g + 128] = jnp.take_along_axis(tile, (8 * g) % 128 + lane // 16, axis=1)
    diagonal = (iota((16, 256), 1) % 16) == iota((16, 256), 0)

    proj[...] = jnp.zeros((NPC * 16, 2 * NZ), F32)

    def halo_x(up):
        return pltpu.make_async_remote_copy(
            section.at[:, LX - 1 if up else 0], sec.at[:, 0 if up else LX + 1, pl.ds(8, LY)],
            xs.at[0 if up else 1], xr.at[0 if up else 1],
            device_id={"gx": gx + 1 if up else gx - 1}, device_id_type=MESH,
        )

    def halo_y(up):
        return pltpu.make_async_remote_copy(
            edges.at[:, :, LY - 1 if up else 0], ylo if up else yhi,
            ys.at[0 if up else 1], yr.at[0 if up else 1],
            device_id={"gy": gy + 1 if up else gy - 1}, device_id_type=MESH,
        )

    def regress(c, aside):
        n = 8 * PAIRS
        ones = (iota((32, NZ), 0) < 3).astype(F32).astype(BF)
        bias2 = jnp.concatenate([b2c[...]] * 4, axis=1)
        bias3 = jnp.concatenate([b3c[...]] * 4, axis=1)
        cells, first, second = {}, {}, {}
        for t in range(n + 2 * LAG):
            if t < n:
                if t % 8 == 0:
                    parts = []
                    for dx in range(2):
                        for o in range(2):
                            v = sec[:, CH * c + 1 + 2 * (t // 8) + dx, 8 + 8 * o : 16 + 8 * o, :]
                            parts.append(jnp.concatenate([v.reshape(96, NZ).astype(BF), ones], axis=0))
                    cells[t // 8] = jnp.concatenate(parts, axis=1)
                one = jnp.dot(w1s[t % 8], cells[t // 8], preferred_element_type=F32)
            if LAG <= t < n + LAG:
                two = jnp.dot(w2v[...], first.pop(t - LAG), preferred_element_type=F32)
            if t >= 2 * LAG:
                u = t - 2 * LAG
                three = jnp.dot(w3p[...], second.pop(u), preferred_element_type=F32) + bias3
                for dx in range(2):
                    for o in range(2):
                        h = 2 * dx + o
                        chem[CH * c + 2 * (u // 8) + dx, o, pl.ds(u % 8, 16, stride=9), :] = three[:, NZ * h : NZ * h + NZ]
            if t < n:
                first[t] = jnp.tanh(one).astype(BF)
            if LAG <= t < n + LAG:
                second[t - LAG] = jnp.tanh(two + bias2).astype(BF)
            aside(t)

    lane3 = iota((LY, NZ), 1)

    def combine(x, extra=None):
        e = x + 1
        sec[:, e, 7:8, :] = ylo[:, x]
        sec[:, e, 24:25, :] = yhi[:, x]
        d = diffv[x] * (0.25 * DT)
        vx, vy, vz = (velv[i, x] * (-0.125 * DT) for i in range(3))
        up = jnp.where(lane3 == NZ - 1, 0.0, d + vz)
        down = jnp.where(lane3 == 0, 0.0, d - vz)
        c = sec[:, e, 8:24, :]
        total = 0.75 * basev[:, x] + (0.25 - 6.0 * d) * c
        total += (d + vx) * sec[:, e + 1, 8:24, :] + (d - vx) * sec[:, e - 1, 8:24, :]
        total += (d + vy) * sec[:, e, 9:25, :] + (d - vy) * sec[:, e, 7:23, :]
        total += up * pltpu.roll(c, NZ - 1, axis=2) + down * pltpu.roll(c, 1, axis=2)
        if extra is not None:
            total += spr[extra]
        for k in range(NPC):
            for o in range(2):
                result[k, x, 8 * o : 8 * o + 8, :] = total[k, 8 * o : 8 * o + 8] + chem[x, o, 9 * k : 9 * k + 8, :]

    def project(c):
        left = []
        for k in range(NPC):
            line = lrep[k : k + 1, pl.ds(pl.multiple_of(256 * c, 256), 256)]
            left.append(jnp.where(diagonal, jnp.broadcast_to(line, (16, 256)), 0.0).astype(BF))
        right = [par[pl.ds(16 * c, 16), 16 * h : 16 * h + 16, :].reshape(256, NZ) for h in range(2)]
        return jnp.dot(jnp.concatenate(left, axis=0), jnp.concatenate(right, axis=1), preferred_element_type=F32)

    def open_step(b, carry):
        chunk_copy(b + 1).wait()
        parcel_copy(b + 1).wait()
        got = []

        def aside(t):
            if t % 3 == 2 and len(got) < 5:
                got.append(project(5 * b + len(got)))

        regress(b + 1, aside)
        proj[...] += sum(got)
        return carry

    parcel_copy(0).wait()
    lax.fori_loop(0, 1, open_step, 0)

    pl.semaphore_wait(barrier, NG - 1 + (gx > 0).astype(jnp.int32) + (gx < NG - 1).astype(jnp.int32))

    pl.when(gy < NG - 1)(lambda: halo_y(True).start())
    pl.when(gy > 0)(lambda: halo_y(False).start())
    pl.when(gx < NG - 1)(lambda: halo_x(True).start())
    pl.when(gx > 0)(lambda: halo_x(False).start())

    lax.fori_loop(1, NCH // 2, open_step, 0)

    projected = proj[...].astype(BF)
    eye = iota((PB, PB), 0) == iota((PB, PB), 1)
    own_row = jnp.broadcast_to(ownv[...].astype(F32), (PB, PB))
    own_col = jnp.sum(jnp.where(eye, own_row, 0.0), axis=1, keepdims=True)
    earlier = (own_row == own_col) & (iota((PB, PB), 0) < iota((PB, PB), 1))
    rank = jnp.sum(jnp.where(earlier, 1.0, 0.0), axis=0, keepdims=True)
    slot = jnp.broadcast_to(ownv[...].astype(F32) * CAP + rank, (NG * CAP, PB))
    chosen = (slot == iota((NG * CAP, PB), 0).astype(F32)).astype(F32).astype(BF)
    blk_row = jnp.broadcast_to(blkv[...].astype(F32) + 1.0, (PB, PB))
    tag = jnp.broadcast_to(jnp.sum(jnp.where(eye, blk_row, 0.0), axis=1, keepdims=True), (PB, NZ)).astype(BF)
    pieces = [
        jnp.concatenate([projected[16 * k : 16 * k + 16, 0:NZ], projected[16 * k : 16 * k + 16, NZ : 2 * NZ]], axis=0)
        for k in range(NPC)
    ]
    values = jnp.dot(chosen, jnp.concatenate(pieces + [tag], axis=1), preferred_element_type=F32)
    for i in range(NG):
        send[i] = values[CAP * i : CAP * i + CAP, :]
    recv[gy] = send[gy]

    def exchange(d):
        peer = lax.rem(gy + d, NG)
        return pltpu.make_async_remote_copy(
            send.at[peer], recv.at[gy], ssem.at[d], rsem.at[d], device_id={"gy": peer}, device_id_type=MESH
        )

    for d in range(1, NG):
        exchange(d).start()

    @pl.when(gx > 0)
    def _():
        halo_x(True).wait_recv()

    @pl.when(gx == 0)
    def _():
        sec[:, 0, 8:24, :] = jnp.zeros((NPC, LY, NZ), F32)

    @pl.when(gx < NG - 1)
    def _():
        halo_x(False).wait_recv()

    @pl.when(gx == NG - 1)
    def _():
        sec[:, LX + 1, 8:24, :] = jnp.zeros((NPC, LY, NZ), F32)

    @pl.when(gy > 0)
    def _():
        halo_y(True).wait_recv()

    @pl.when(gy == 0)
    def _():
        ylo[...] = jnp.zeros((NPC, LX, 1, NZ), F32)

    @pl.when(gy < NG - 1)
    def _():
        halo_y(False).wait_recv()

    @pl.when(gy == NG - 1)
    def _():
        yhi[...] = jnp.zeros((NPC, LX, 1, NZ), F32)

    for c in (5, 6, 7, 0):
        chunk_copy(c).wait()
    for c in big:
        c.wait()

    def step(b, carry):
        @pl.when(b == NCH - 1)
        def _():
            for d in range(1, NG):
                exchange(d).wait_recv()
            got = jnp.concatenate([recv[i] for i in range(NG)], axis=0)
            place = (got[:, NPC * NZ :] - 1.0 == iota((NG * CAP, NZ), 1).astype(F32)).astype(F32).T[0:SB].astype(BF)
            mine = jnp.dot(place, got[:, 0 : NPC * NZ].astype(BF), preferred_element_type=F32) * (0.25 * DT)
            for k in range(NPC):
                for x in range(2):
                    spr[x, k] = mine[LY * x : LY * x + LY, NZ * k : NZ * k + NZ]

        late, early = 2 * b - NCH + 1, jnp.maximum(2 * b - NCH, 1)

        def aside(t):
            if t % 2 == 1 and t // 2 < 2 * CH:
                i = t // 2
                combine(CH * (early if i < CH else late) + i % CH)

        chunk = lax.rem(b + 1, NCH)
        regress(chunk, aside)
        return carry

    lax.fori_loop(NCH // 2, NCH, step, 0)
    for x in range(CH):
        combine(x, x if x < 2 else None)
    for d in range(1, NG):
        exchange(d).wait_send()
    pl.when(gy < NG - 1)(lambda: halo_y(True).wait_send())
    pl.when(gy > 0)(lambda: halo_y(False).wait_send())
    pl.when(gx < NG - 1)(lambda: halo_x(True).wait_send())
    pl.when(gx > 0)(lambda: halo_x(False).wait_send())


def shards(
    base_scores, section_scores, velocity, diffusivity, w_first, b_first, w_second, b_second, w_third, b_third,
    loadings, parcel_species, parcel_owner, parcel_block,
):
    anywhere = pl.BlockSpec(memory_space=pltpu.HBM)
    vmem = pltpu.VMEM
    dma = pltpu.SemaphoreType.DMA
    return pl.pallas_call(
        kernel,
        out_shape=jax.ShapeDtypeStruct((NPC, LX, LY, NZ), F32),
        in_specs=[anywhere] * 15,
        out_specs=pl.BlockSpec(memory_space=pltpu.VMEM),
        scratch_shapes=[
            vmem((NPC, LX + 2, 2 * LY, NZ), F32),
            vmem((NPC, LX, LY, NZ), F32),
            vmem((3, LX, LY, NZ), F32),
            vmem((LX, LY, NZ), F32),
            vmem((LX, 2, CROWS, NZ), F32),
            vmem((SPAD, PB, NZ), BF),
            vmem((NPC * 16, 2 * NZ), F32),
            vmem((16, SPAD * 16), F32),
            vmem((16, 384), F32),
            vmem((NPC, LX, 1, NZ), F32),
            vmem((NPC, LX, 1, NZ), F32),
            vmem((NG, CAP, WIDE), F32),
            vmem((NG, CAP, WIDE), F32),
            vmem((2, NPC, LY, NZ), F32),
            vmem((NPC, HID), BF),
            vmem((1, HID), F32),
            vmem((HID, HID), BF),
            vmem((1, HID), F32),
            vmem((NPC, HID), BF),
            vmem((1, PB), jnp.int32),
            vmem((1, PB), jnp.int32),
            vmem((NPC, SPEC), BF),
            pltpu.SMEM((1, NPC), F32),
            vmem((16, HID), F32),
            vmem((8, HID, NZ), BF),
            vmem((HID, NZ), F32),
            vmem((16, HID), BF),
            vmem((16, NZ), F32),
            dma((12,)),
            dma((SPEC // PART,)),
            dma((NCH,)),
            dma((2,)),
            dma((2,)),
            dma((2,)),
            dma((2,)),
            dma((NG,)),
            dma((NG,)),
        ],
        compiler_params=pltpu.CompilerParams(collective_id=0, has_side_effects=True, vmem_limit_bytes=40 * 1024 * 1024),
        name="section_step",
    )(*[pltpu.with_memory_space_constraint(v, pltpu.HBM) for v in (
        base_scores, section_scores, section_scores.reshape(NPC, LX, LY, 1, NZ), velocity, diffusivity,
        w_first.T, b_first.reshape(1, HID), w_second, b_second.reshape(1, HID), w_third, b_third.reshape(1, NPC),
        loadings, parcel_species.transpose(1, 0, 2), parcel_owner.reshape(1, PB), parcel_block.reshape(1, PB),
    )])


def solution(mesh):
    placed = (
        P(None, "gx", "gy", None), P(None, "gx", "gy", None), P(None, "gx", "gy", None), P("gx", "gy", None),
        P(), P(), P(), P(), P(), P(), P(),
        P(("gx", "gy"), None, None), P(("gx", "gy"), None), P(("gx", "gy")),
    )
    return jax.shard_map(
        shards, mesh=mesh, in_specs=placed, out_specs=P(None, "gx", "gy", None), check_vma=False
    )
```

```python
import jax
import jax.numpy as jnp
from jax import lax
from jax.experimental import pallas as pl
from jax.experimental.pallas import tpu as pltpu
from jax.sharding import PartitionSpec as P

BF = jnp.bfloat16
F32 = jnp.float32
MESH = pl.DeviceIdType.MESH

NPC = 12
SPEC = 300
SPAD = 320
PART = 60
HID = 256
LX, LY, NZ = 32, 16, 128
PB = 32
CAP = 4
SB = 32
NG = 16
CH = 4
NCH = LX // CH
PAIRS = CH // 2
DT = 0.25
WIDE = (NPC + 1) * NZ
CROWS = 144


def iota(shape, dim):
    return lax.broadcasted_iota(jnp.int32, shape, dim)


def kernel(
    base, section, edges, velocity, diffusivity, w1t, b1, w2, b2, w3, b3, loadings, parcels, owner, block,
    result,
    sec, basev, velv, diffv, chem, par, proj, lrep, lpad, ylo, yhi, send, recv, spr,
    w1tv, b1v, w2v, b2v, w3v, ownv, blkv, loadv, b3s, a16, w1s, b2c, w3p, b3c,
    in_sem, par_sem, chunk_sem, xs, xr, ys, yr, ssem, rsem,
):
    gx = lax.axis_index("gx")
    gy = lax.axis_index("gy")

    barrier = pltpu.get_barrier_semaphore()
    for d in range(1, NG):
        pl.semaphore_signal(barrier, inc=1, device_id={"gy": lax.rem(gy + d, NG)}, device_id_type=MESH)

    @pl.when(gx > 0)
    def _():
        pl.semaphore_signal(barrier, inc=1, device_id={"gx": gx - 1}, device_id_type=MESH)

    @pl.when(gx < NG - 1)
    def _():
        pl.semaphore_signal(barrier, inc=1, device_id={"gx": gx + 1}, device_id_type=MESH)

    small = [
        pltpu.make_async_copy(a, b, in_sem.at[i])
        for i, (a, b) in enumerate(
            [(w1t, w1tv), (b1, b1v), (w2, w2v), (b2, b2v), (w3, w3v), (b3, b3s), (loadings, loadv), (owner, ownv), (block, blkv)]
        )
    ]
    for c in small:
        c.start()

    def chunk_copy(c):
        return pltpu.make_async_copy(
            section.at[:, pl.ds(CH * c, CH)], sec.at[:, pl.ds(1 + CH * c, CH), pl.ds(8, LY)], chunk_sem.at[c]
        )

    def parcel_copy(i):
        return pltpu.make_async_copy(parcels.at[pl.ds(PART * i, PART)], par.at[pl.ds(PART * i, PART)], par_sem.at[i])

    chunk_copy(1).start()
    parcel_copy(0).start()
    parcel_copy(1).start()
    chunk_copy(2).start()
    parcel_copy(2).start()
    chunk_copy(3).start()
    parcel_copy(3).start()
    chunk_copy(4).start()
    parcel_copy(4).start()
    for c in (5, 6, 7, 0):
        chunk_copy(c).start()
    big = [
        pltpu.make_async_copy(a, b, in_sem.at[9 + i])
        for i, (a, b) in enumerate([(velocity, velv), (diffusivity, diffv), (base, basev)])
    ]
    for c in big:
        c.start()

    for c in small:
        c.wait()
    par[SPEC:SPAD] = jnp.zeros((SPAD - SPEC, PB, NZ), BF)
    bias = b1v[...]
    hi = bias.astype(BF).astype(F32)
    mid = (bias - hi).astype(BF).astype(F32)
    a16[0:NPC, :] = w1tv[...].astype(F32)
    a16[12:13, :] = hi
    a16[13:14, :] = mid
    a16[14:15, :] = (bias - hi) - mid
    a16[15:16, :] = jnp.zeros((1, HID), F32)
    left = a16[...].T.astype(BF)
    row, lane = iota((16, NZ), 0), iota((16, NZ), 1)
    for j in range(8):
        pick = ((lane < 96) & (lane // 8 == row) & (lane % 8 == j)) | ((lane >= 96) & (lane - 96 + 12 == row) & (row < 15))
        w1s[j] = jnp.dot(left, pick.astype(F32).astype(BF), preferred_element_type=F32).astype(BF)
    b2c[...] = jnp.broadcast_to(b2v[...], (NZ, HID)).T
    w3p[...] = jnp.zeros((16, HID), BF)
    w3p[0:NPC, :] = (w3v[...].astype(F32) * (0.25 * DT)).astype(BF)
    col = jnp.zeros((16, NZ), F32)
    for k in range(NPC):
        col = jnp.where(row == k, b3s[0, k] * (0.25 * DT), col)
    b3c[...] = col
    lpad[...] = jnp.zeros((16, 384), F32)
    lpad[0:NPC, 0:SPEC] = loadv[...].astype(F32)
    for g in range(SPAD // 8):
        tile = lpad[:, (8 * g // 128) * 128 : (8 * g // 128) * 128 + 128]
        lrep[:, 128 * g : 128 * g + 128] = jnp.take_along_axis(tile, (8 * g) % 128 + lane // 16, axis=1)
    diagonal = (iota((16, 256), 1) % 16) == iota((16, 256), 0)

    proj[...] = jnp.zeros((NPC * 16, 2 * NZ), F32)

    def halo_x(up):
        return pltpu.make_async_remote_copy(
            section.at[:, LX - 1 if up else 0], sec.at[:, 0 if up else LX + 1, pl.ds(8, LY)],
            xs.at[0 if up else 1], xr.at[0 if up else 1],
            device_id={"gx": gx + 1 if up else gx - 1}, device_id_type=MESH,
        )

    def halo_y(up):
        return pltpu.make_async_remote_copy(
            edges.at[:, :, LY - 1 if up else 0], ylo if up else yhi,
            ys.at[0 if up else 1], yr.at[0 if up else 1],
            device_id={"gy": gy + 1 if up else gy - 1}, device_id_type=MESH,
        )

    def regress(c, aside):
        n = 8 * PAIRS
        ones = (iota((32, NZ), 0) < 3).astype(F32).astype(BF)
        bias2 = jnp.concatenate([b2c[...]] * 4, axis=1)
        bias3 = jnp.concatenate([b3c[...]] * 4, axis=1)
        cells, first, second = {}, {}, {}
        for t in range(n + 3):
            if t >= 3:
                u = t - 3
                three = jnp.dot(w3p[...], second.pop(u), preferred_element_type=F32) + bias3
                for dx in range(2):
                    for o in range(2):
                        h = 2 * dx + o
                        chem[CH * c + 2 * (u // 8) + dx, o, pl.ds(u % 8, 16, stride=9), :] = three[:, NZ * h : NZ * h + NZ]
            if t < n:
                if t % 8 == 0:
                    parts = []
                    for dx in range(2):
                        for o in range(2):
                            v = sec[:, CH * c + 1 + 2 * (t // 8) + dx, 8 + 8 * o : 16 + 8 * o, :]
                            parts.append(jnp.concatenate([v.reshape(96, NZ).astype(BF), ones], axis=0))
                    cells[t // 8] = jnp.concatenate(parts, axis=1)
                one = jnp.dot(w1s[t % 8], cells[t // 8], preferred_element_type=F32)
                first[t] = jnp.tanh(one).astype(BF)
            if 1 <= t <= n:
                two = jnp.dot(w2v[...], first.pop(t - 1), preferred_element_type=F32)
                second[t - 1] = jnp.tanh(two + bias2).astype(BF)
            aside(t)

    lane3 = iota((LY, NZ), 1)

    def combine(x, extra=None):
        e = x + 1
        sec[:, e, 7:8, :] = ylo[:, x]
        sec[:, e, 24:25, :] = yhi[:, x]
        d = diffv[x] * (0.25 * DT)
        vx, vy, vz = (velv[i, x] * (-0.125 * DT) for i in range(3))
        up = jnp.where(lane3 == NZ - 1, 0.0, d + vz)
        down = jnp.where(lane3 == 0, 0.0, d - vz)
        c = sec[:, e, 8:24, :]
        total = 0.75 * basev[:, x] + (0.25 - 6.0 * d) * c
        total += (d + vx) * sec[:, e + 1, 8:24, :] + (d - vx) * sec[:, e - 1, 8:24, :]
        total += (d + vy) * sec[:, e, 9:25, :] + (d - vy) * sec[:, e, 7:23, :]
        total += up * pltpu.roll(c, NZ - 1, axis=2) + down * pltpu.roll(c, 1, axis=2)
        if extra is not None:
            total += spr[extra]
        for k in range(NPC):
            for o in range(2):
                result[k, x, 8 * o : 8 * o + 8, :] = total[k, 8 * o : 8 * o + 8] + chem[x, o, 9 * k : 9 * k + 8, :]

    def project(c):
        left = []
        for k in range(NPC):
            line = lrep[k : k + 1, pl.ds(pl.multiple_of(256 * c, 256), 256)]
            left.append(jnp.where(diagonal, jnp.broadcast_to(line, (16, 256)), 0.0).astype(BF))
        right = [par[pl.ds(16 * c, 16), 16 * h : 16 * h + 16, :].reshape(256, NZ) for h in range(2)]
        return jnp.dot(jnp.concatenate(left, axis=0), jnp.concatenate(right, axis=1), preferred_element_type=F32)

    def open_step(b, carry):
        chunk_copy(b + 1).wait()
        parcel_copy(b + 1).wait()
        got = []

        def aside(t):
            if t % 3 == 2 and len(got) < 5:
                got.append(project(5 * b + len(got)))

        regress(b + 1, aside)
        proj[...] += sum(got)
        return carry

    parcel_copy(0).wait()
    lax.fori_loop(0, 1, open_step, 0)

    pl.semaphore_wait(barrier, NG - 1 + (gx > 0).astype(jnp.int32) + (gx < NG - 1).astype(jnp.int32))

    pl.when(gy < NG - 1)(lambda: halo_y(True).start())
    pl.when(gy > 0)(lambda: halo_y(False).start())
    pl.when(gx < NG - 1)(lambda: halo_x(True).start())
    pl.when(gx > 0)(lambda: halo_x(False).start())

    lax.fori_loop(1, NCH // 2, open_step, 0)

    projected = proj[...].astype(BF)
    eye = iota((PB, PB), 0) == iota((PB, PB), 1)
    own_row = jnp.broadcast_to(ownv[...].astype(F32), (PB, PB))
    own_col = jnp.sum(jnp.where(eye, own_row, 0.0), axis=1, keepdims=True)
    earlier = (own_row == own_col) & (iota((PB, PB), 0) < iota((PB, PB), 1))
    rank = jnp.sum(jnp.where(earlier, 1.0, 0.0), axis=0, keepdims=True)
    slot = jnp.broadcast_to(ownv[...].astype(F32) * CAP + rank, (NG * CAP, PB))
    chosen = (slot == iota((NG * CAP, PB), 0).astype(F32)).astype(F32).astype(BF)
    blk_row = jnp.broadcast_to(blkv[...].astype(F32) + 1.0, (PB, PB))
    tag = jnp.broadcast_to(jnp.sum(jnp.where(eye, blk_row, 0.0), axis=1, keepdims=True), (PB, NZ)).astype(BF)
    pieces = [
        jnp.concatenate([projected[16 * k : 16 * k + 16, 0:NZ], projected[16 * k : 16 * k + 16, NZ : 2 * NZ]], axis=0)
        for k in range(NPC)
    ]
    values = jnp.dot(chosen, jnp.concatenate(pieces + [tag], axis=1), preferred_element_type=F32)
    for i in range(NG):
        send[i] = values[CAP * i : CAP * i + CAP, :]
    recv[gy] = send[gy]

    def exchange(d):
        peer = lax.rem(gy + d, NG)
        return pltpu.make_async_remote_copy(
            send.at[peer], recv.at[gy], ssem.at[d], rsem.at[d], device_id={"gy": peer}, device_id_type=MESH
        )

    for d in range(1, NG):
        exchange(d).start()

    @pl.when(gx > 0)
    def _():
        halo_x(True).wait_recv()

    @pl.when(gx == 0)
    def _():
        sec[:, 0, 8:24, :] = jnp.zeros((NPC, LY, NZ), F32)

    @pl.when(gx < NG - 1)
    def _():
        halo_x(False).wait_recv()

    @pl.when(gx == NG - 1)
    def _():
        sec[:, LX + 1, 8:24, :] = jnp.zeros((NPC, LY, NZ), F32)

    @pl.when(gy > 0)
    def _():
        halo_y(True).wait_recv()

    @pl.when(gy == 0)
    def _():
        ylo[...] = jnp.zeros((NPC, LX, 1, NZ), F32)

    @pl.when(gy < NG - 1)
    def _():
        halo_y(False).wait_recv()

    @pl.when(gy == NG - 1)
    def _():
        yhi[...] = jnp.zeros((NPC, LX, 1, NZ), F32)

    for c in (5, 6, 7, 0):
        chunk_copy(c).wait()
    for c in big:
        c.wait()

    def step(b, carry):
        @pl.when(b == NCH - 1)
        def _():
            for d in range(1, NG):
                exchange(d).wait_recv()
            got = jnp.concatenate([recv[i] for i in range(NG)], axis=0)
            place = (got[:, NPC * NZ :] - 1.0 == iota((NG * CAP, NZ), 1).astype(F32)).astype(F32).T[0:SB].astype(BF)
            mine = jnp.dot(place, got[:, 0 : NPC * NZ].astype(BF), preferred_element_type=F32) * (0.25 * DT)
            for k in range(NPC):
                for x in range(2):
                    spr[x, k] = mine[LY * x : LY * x + LY, NZ * k : NZ * k + NZ]

        late, early = 2 * b - NCH + 1, jnp.maximum(2 * b - NCH, 1)

        def aside(t):
            if t % 2 == 1 and t // 2 < 2 * CH:
                i = t // 2
                combine(CH * (early if i < CH else late) + i % CH)

        chunk = lax.rem(b + 1, NCH)
        regress(chunk, aside)
        return carry

    lax.fori_loop(NCH // 2, NCH, step, 0)
    for x in range(CH):
        combine(x, x if x < 2 else None)
    for d in range(1, NG):
        exchange(d).wait_send()
    pl.when(gy < NG - 1)(lambda: halo_y(True).wait_send())
    pl.when(gy > 0)(lambda: halo_y(False).wait_send())
    pl.when(gx < NG - 1)(lambda: halo_x(True).wait_send())
    pl.when(gx > 0)(lambda: halo_x(False).wait_send())


def shards(
    base_scores, section_scores, velocity, diffusivity, w_first, b_first, w_second, b_second, w_third, b_third,
    loadings, parcel_species, parcel_owner, parcel_block,
):
    anywhere = pl.BlockSpec(memory_space=pltpu.HBM)
    vmem = pltpu.VMEM
    dma = pltpu.SemaphoreType.DMA
    return pl.pallas_call(
        kernel,
        out_shape=jax.ShapeDtypeStruct((NPC, LX, LY, NZ), F32),
        in_specs=[anywhere] * 15,
        out_specs=pl.BlockSpec(memory_space=pltpu.VMEM),
        scratch_shapes=[
            vmem((NPC, LX + 2, 2 * LY, NZ), F32),
            vmem((NPC, LX, LY, NZ), F32),
            vmem((3, LX, LY, NZ), F32),
            vmem((LX, LY, NZ), F32),
            vmem((LX, 2, CROWS, NZ), F32),
            vmem((SPAD, PB, NZ), BF),
            vmem((NPC * 16, 2 * NZ), F32),
            vmem((16, SPAD * 16), F32),
            vmem((16, 384), F32),
            vmem((NPC, LX, 1, NZ), F32),
            vmem((NPC, LX, 1, NZ), F32),
            vmem((NG, CAP, WIDE), F32),
            vmem((NG, CAP, WIDE), F32),
            vmem((2, NPC, LY, NZ), F32),
            vmem((NPC, HID), BF),
            vmem((1, HID), F32),
            vmem((HID, HID), BF),
            vmem((1, HID), F32),
            vmem((NPC, HID), BF),
            vmem((1, PB), jnp.int32),
            vmem((1, PB), jnp.int32),
            vmem((NPC, SPEC), BF),
            pltpu.SMEM((1, NPC), F32),
            vmem((16, HID), F32),
            vmem((8, HID, NZ), BF),
            vmem((HID, NZ), F32),
            vmem((16, HID), BF),
            vmem((16, NZ), F32),
            dma((12,)),
            dma((SPEC // PART,)),
            dma((NCH,)),
            dma((2,)),
            dma((2,)),
            dma((2,)),
            dma((2,)),
            dma((NG,)),
            dma((NG,)),
        ],
        compiler_params=pltpu.CompilerParams(collective_id=0, has_side_effects=True, vmem_limit_bytes=40 * 1024 * 1024),
        name="section_step",
    )(*[pltpu.with_memory_space_constraint(v, pltpu.HBM) for v in (
        base_scores, section_scores, section_scores.reshape(NPC, LX, LY, 1, NZ), velocity, diffusivity,
        w_first.T, b_first.reshape(1, HID), w_second, b_second.reshape(1, HID), w_third, b_third.reshape(1, NPC),
        loadings, parcel_species.transpose(1, 0, 2), parcel_owner.reshape(1, PB), parcel_block.reshape(1, PB),
    )])


def solution(mesh):
    placed = (
        P(None, "gx", "gy", None), P(None, "gx", "gy", None), P(None, "gx", "gy", None), P("gx", "gy", None),
        P(), P(), P(), P(), P(), P(), P(),
        P(("gx", "gy"), None, None), P(("gx", "gy"), None), P(("gx", "gy")),
    )
    return jax.shard_map(
        shards, mesh=mesh, in_specs=placed, out_specs=P(None, "gx", "gy", None), check_vma=False
    )
```

```python
import jax
import jax.numpy as jnp
from jax import lax
from jax.experimental import pallas as pl
from jax.experimental.pallas import tpu as pltpu
from jax.sharding import PartitionSpec as P

BF = jnp.bfloat16
F32 = jnp.float32
MESH = pl.DeviceIdType.MESH

NPC = 12
SPEC = 300
SPAD = 320
PART = 60
HID = 256
LX, LY, NZ = 32, 16, 128
PB = 32
CAP = 4
SB = 32
NG = 16
CH = 4
NCH = LX // CH
PAIRS = CH // 2
DT = 0.25
WIDE = (NPC + 1) * NZ
CROWS = 144


def iota(shape, dim):
    return lax.broadcasted_iota(jnp.int32, shape, dim)


def kernel(
    base, section, edges, velocity, diffusivity, w1t, b1, w2, b2, w3, b3, loadings, parcels, owner, block,
    result,
    sec, basev, velv, diffv, chem, par, proj, lrep, lpad, ylo, yhi, send, recv, spr,
    w1tv, b1v, w2v, b2v, w3v, ownv, blkv, loadv, b3s, a16, w1s, b2c, w3p, b3c, rest,
    in_sem, par_sem, chunk_sem, xs, xr, ys, yr, ssem, rsem,
):
    gx = lax.axis_index("gx")
    gy = lax.axis_index("gy")

    barrier = pltpu.get_barrier_semaphore()
    for d in range(1, NG):
        pl.semaphore_signal(barrier, inc=1, device_id={"gy": lax.rem(gy + d, NG)}, device_id_type=MESH)

    @pl.when(gx > 0)
    def _():
        pl.semaphore_signal(barrier, inc=1, device_id={"gx": gx - 1}, device_id_type=MESH)

    @pl.when(gx < NG - 1)
    def _():
        pl.semaphore_signal(barrier, inc=1, device_id={"gx": gx + 1}, device_id_type=MESH)

    small = [
        pltpu.make_async_copy(a, b, in_sem.at[i])
        for i, (a, b) in enumerate(
            [(w1t, w1tv), (b1, b1v), (w2, w2v), (b2, b2v), (w3, w3v), (b3, b3s), (loadings, loadv), (owner, ownv), (block, blkv)]
        )
    ]
    for c in small:
        c.start()

    def chunk_copy(c):
        return pltpu.make_async_copy(
            section.at[:, pl.ds(CH * c, CH)], sec.at[:, pl.ds(1 + CH * c, CH), pl.ds(8, LY)], chunk_sem.at[c]
        )

    def parcel_copy(i):
        return pltpu.make_async_copy(parcels.at[pl.ds(PART * i, PART)], par.at[pl.ds(PART * i, PART)], par_sem.at[i])

    chunk_copy(1).start()
    parcel_copy(0).start()
    parcel_copy(1).start()
    chunk_copy(2).start()
    parcel_copy(2).start()
    chunk_copy(3).start()
    parcel_copy(3).start()
    chunk_copy(4).start()
    parcel_copy(4).start()
    for c in (5, 6, 7, 0):
        chunk_copy(c).start()
    big = [
        pltpu.make_async_copy(a, b, in_sem.at[9 + i])
        for i, (a, b) in enumerate([(velocity, velv), (diffusivity, diffv), (base, basev)])
    ]
    for c in big:
        c.start()

    for c in small:
        c.wait()
    par[SPEC:SPAD] = jnp.zeros((SPAD - SPEC, PB, NZ), BF)
    bias = b1v[...]
    hi = bias.astype(BF).astype(F32)
    mid = (bias - hi).astype(BF).astype(F32)
    a16[0:NPC, :] = w1tv[...].astype(F32)
    a16[12:13, :] = hi
    a16[13:14, :] = mid
    a16[14:15, :] = (bias - hi) - mid
    a16[15:16, :] = jnp.zeros((1, HID), F32)
    left = a16[...].T.astype(BF)
    row, lane = iota((16, NZ), 0), iota((16, NZ), 1)
    for j in range(8):
        pick = ((lane < 96) & (lane // 8 == row) & (lane % 8 == j)) | ((lane >= 96) & (lane - 96 + 12 == row) & (row < 15))
        w1s[j] = jnp.dot(left, pick.astype(F32).astype(BF), preferred_element_type=F32).astype(BF)
    b2c[...] = jnp.broadcast_to(b2v[...], (NZ, HID)).T
    w3p[...] = jnp.zeros((64, HID), BF)
    w3p[0:NPC, :] = (w3v[...].astype(F32) * (0.25 * DT)).astype(BF)
    col = jnp.zeros((16, NZ), F32)
    for k in range(NPC):
        col = jnp.where(row == k, b3s[0, k] * (0.25 * DT), col)
    b3c[...] = col
    lpad[...] = jnp.zeros((16, 384), F32)
    lpad[0:NPC, 0:SPEC] = loadv[...].astype(F32)
    for g in range(SPAD // 8):
        tile = lpad[:, (8 * g // 128) * 128 : (8 * g // 128) * 128 + 128]
        lrep[:, 128 * g : 128 * g + 128] = jnp.take_along_axis(tile, (8 * g) % 128 + lane // 16, axis=1)
    diagonal = (iota((16, 256), 1) % 16) == iota((16, 256), 0)

    proj[...] = jnp.zeros((NPC * 16, 2 * NZ), F32)

    def halo_x(up):
        return pltpu.make_async_remote_copy(
            section.at[:, LX - 1 if up else 0], sec.at[:, 0 if up else LX + 1, pl.ds(8, LY)],
            xs.at[0 if up else 1], xr.at[0 if up else 1],
            device_id={"gx": gx + 1 if up else gx - 1}, device_id_type=MESH,
        )

    def halo_y(up):
        return pltpu.make_async_remote_copy(
            edges.at[:, :, LY - 1 if up else 0], ylo if up else yhi,
            ys.at[0 if up else 1], yr.at[0 if up else 1],
            device_id={"gy": gy + 1 if up else gy - 1}, device_id_type=MESH,
        )

    def regress(c, aside):
        n = 8 * PAIRS
        ones = (iota((32, NZ), 0) < 3).astype(F32).astype(BF)
        bias2 = jnp.concatenate([b2c[...]] * 4, axis=1)
        bias3 = jnp.concatenate([b3c[...]] * 4, axis=1)
        cells, first, second = {}, {}, {}
        for t in range(n + 3):
            if t >= 3:
                u = t - 3
                three = jnp.dot(w3p[...], second.pop(u), preferred_element_type=F32)
                rest[...] = three[16:, :]
                three = three[:16, :] + bias3
                for dx in range(2):
                    for o in range(2):
                        h = 2 * dx + o
                        chem[CH * c + 2 * (u // 8) + dx, o, pl.ds(u % 8, 16, stride=9), :] = three[:, NZ * h : NZ * h + NZ]
            if t < n:
                if t % 8 == 0:
                    parts = []
                    for dx in range(2):
                        for o in range(2):
                            v = sec[:, CH * c + 1 + 2 * (t // 8) + dx, 8 + 8 * o : 16 + 8 * o, :]
                            parts.append(jnp.concatenate([v.reshape(96, NZ).astype(BF), ones], axis=0))
                    cells[t // 8] = jnp.concatenate(parts, axis=1)
                one = jnp.dot(w1s[t % 8], cells[t // 8], preferred_element_type=F32)
                first[t] = jnp.tanh(one).astype(BF)
            if 1 <= t <= n:
                two = jnp.dot(w2v[...], first.pop(t - 1), preferred_element_type=F32)
                second[t - 1] = jnp.tanh(two + bias2).astype(BF)
            aside(t)

    lane3 = iota((LY, NZ), 1)

    def combine(x, extra=None):
        e = x + 1
        sec[:, e, 7:8, :] = ylo[:, x]
        sec[:, e, 24:25, :] = yhi[:, x]
        d = diffv[x] * (0.25 * DT)
        vx, vy, vz = (velv[i, x] * (-0.125 * DT) for i in range(3))
        up = jnp.where(lane3 == NZ - 1, 0.0, d + vz)
        down = jnp.where(lane3 == 0, 0.0, d - vz)
        c = sec[:, e, 8:24, :]
        total = 0.75 * basev[:, x] + (0.25 - 6.0 * d) * c
        total += (d + vx) * sec[:, e + 1, 8:24, :] + (d - vx) * sec[:, e - 1, 8:24, :]
        total += (d + vy) * sec[:, e, 9:25, :] + (d - vy) * sec[:, e, 7:23, :]
        total += up * pltpu.roll(c, NZ - 1, axis=2) + down * pltpu.roll(c, 1, axis=2)
        if extra is not None:
            total += spr[extra]
        for k in range(NPC):
            for o in range(2):
                result[k, x, 8 * o : 8 * o + 8, :] = total[k, 8 * o : 8 * o + 8] + chem[x, o, 9 * k : 9 * k + 8, :]

    def project(c):
        left = []
        for k in range(NPC):
            line = lrep[k : k + 1, pl.ds(pl.multiple_of(256 * c, 256), 256)]
            left.append(jnp.where(diagonal, jnp.broadcast_to(line, (16, 256)), 0.0).astype(BF))
        right = [par[pl.ds(16 * c, 16), 16 * h : 16 * h + 16, :].reshape(256, NZ) for h in range(2)]
        right = jnp.concatenate(right, axis=1)
        return jnp.concatenate(
            [jnp.dot(jnp.concatenate(left[i : i + 6], axis=0), right, preferred_element_type=F32) for i in (0, 6)], axis=0
        )

    def open_step(b, carry):
        chunk_copy(b + 1).wait()
        parcel_copy(b + 1).wait()
        got = []

        def aside(t):
            if t == 1:
                for _ in range(5):
                    got.append(project(5 * b + len(got)))

        regress(b + 1, aside)
        proj[...] += sum(got)
        return carry

    parcel_copy(0).wait()
    lax.fori_loop(0, 1, open_step, 0)

    pl.semaphore_wait(barrier, NG - 1 + (gx > 0).astype(jnp.int32) + (gx < NG - 1).astype(jnp.int32))

    pl.when(gy < NG - 1)(lambda: halo_y(True).start())
    pl.when(gy > 0)(lambda: halo_y(False).start())
    pl.when(gx < NG - 1)(lambda: halo_x(True).start())
    pl.when(gx > 0)(lambda: halo_x(False).start())

    lax.fori_loop(1, NCH // 2, open_step, 0)

    projected = proj[...].astype(BF)
    eye = iota((PB, PB), 0) == iota((PB, PB), 1)
    own_row = jnp.broadcast_to(ownv[...].astype(F32), (PB, PB))
    own_col = jnp.sum(jnp.where(eye, own_row, 0.0), axis=1, keepdims=True)
    earlier = (own_row == own_col) & (iota((PB, PB), 0) < iota((PB, PB), 1))
    rank = jnp.sum(jnp.where(earlier, 1.0, 0.0), axis=0, keepdims=True)
    slot = jnp.broadcast_to(ownv[...].astype(F32) * CAP + rank, (NG * CAP, PB))
    chosen = (slot == iota((NG * CAP, PB), 0).astype(F32)).astype(F32).astype(BF)
    blk_row = jnp.broadcast_to(blkv[...].astype(F32) + 1.0, (PB, PB))
    tag = jnp.broadcast_to(jnp.sum(jnp.where(eye, blk_row, 0.0), axis=1, keepdims=True), (PB, NZ)).astype(BF)
    pieces = [
        jnp.concatenate([projected[16 * k : 16 * k + 16, 0:NZ], projected[16 * k : 16 * k + 16, NZ : 2 * NZ]], axis=0)
        for k in range(NPC)
    ]
    values = jnp.dot(chosen, jnp.concatenate(pieces + [tag], axis=1), preferred_element_type=F32)
    for i in range(NG):
        send[i] = values[CAP * i : CAP * i + CAP, :]
    recv[gy] = send[gy]

    def exchange(d):
        peer = lax.rem(gy + d, NG)
        return pltpu.make_async_remote_copy(
            send.at[peer], recv.at[gy], ssem.at[d], rsem.at[d], device_id={"gy": peer}, device_id_type=MESH
        )

    for d in range(1, NG):
        exchange(d).start()

    @pl.when(gx > 0)
    def _():
        halo_x(True).wait_recv()

    @pl.when(gx == 0)
    def _():
        sec[:, 0, 8:24, :] = jnp.zeros((NPC, LY, NZ), F32)

    @pl.when(gx < NG - 1)
    def _():
        halo_x(False).wait_recv()

    @pl.when(gx == NG - 1)
    def _():
        sec[:, LX + 1, 8:24, :] = jnp.zeros((NPC, LY, NZ), F32)

    @pl.when(gy > 0)
    def _():
        halo_y(True).wait_recv()

    @pl.when(gy == 0)
    def _():
        ylo[...] = jnp.zeros((NPC, LX, 1, NZ), F32)

    @pl.when(gy < NG - 1)
    def _():
        halo_y(False).wait_recv()

    @pl.when(gy == NG - 1)
    def _():
        yhi[...] = jnp.zeros((NPC, LX, 1, NZ), F32)

    for c in (5, 6, 7, 0):
        chunk_copy(c).wait()
    for c in big:
        c.wait()

    def step(b, carry):
        late, early = 2 * b - NCH + 1, jnp.maximum(2 * b - NCH, 1)

        def aside(t):
            if t % 2 == 1 and t // 2 < 2 * CH:
                i = t // 2
                combine(CH * (early if i < CH else late) + i % CH)

        chunk = lax.rem(b + 1, NCH)
        regress(chunk, aside)
        return carry

    lax.fori_loop(NCH // 2, NCH, step, 0)
    for d in range(1, NG):
        exchange(d).wait_recv()
    got = jnp.concatenate([recv[i] for i in range(NG)], axis=0)
    place = (got[:, NPC * NZ :] - 1.0 == iota((NG * CAP, NZ), 1).astype(F32)).astype(F32).T[0:SB].astype(BF)
    mine = jnp.dot(place, got[:, 0 : NPC * NZ].astype(BF), preferred_element_type=F32) * (0.25 * DT)
    for k in range(NPC):
        for x in range(2):
            spr[x, k] = mine[LY * x : LY * x + LY, NZ * k : NZ * k + NZ]
    for x in range(CH):
        combine(x, x if x < 2 else None)
    for d in range(1, NG):
        exchange(d).wait_send()
    pl.when(gy < NG - 1)(lambda: halo_y(True).wait_send())
    pl.when(gy > 0)(lambda: halo_y(False).wait_send())
    pl.when(gx < NG - 1)(lambda: halo_x(True).wait_send())
    pl.when(gx > 0)(lambda: halo_x(False).wait_send())


def shards(
    base_scores, section_scores, velocity, diffusivity, w_first, b_first, w_second, b_second, w_third, b_third,
    loadings, parcel_species, parcel_owner, parcel_block,
):
    anywhere = pl.BlockSpec(memory_space=pltpu.HBM)
    vmem = pltpu.VMEM
    dma = pltpu.SemaphoreType.DMA
    return pl.pallas_call(
        kernel,
        out_shape=jax.ShapeDtypeStruct((NPC, LX, LY, NZ), F32),
        in_specs=[anywhere] * 15,
        out_specs=pl.BlockSpec(memory_space=pltpu.VMEM),
        scratch_shapes=[
            vmem((NPC, LX + 2, 2 * LY, NZ), F32),
            vmem((NPC, LX, LY, NZ), F32),
            vmem((3, LX, LY, NZ), F32),
            vmem((LX, LY, NZ), F32),
            vmem((LX, 2, CROWS, NZ), F32),
            vmem((SPAD, PB, NZ), BF),
            vmem((NPC * 16, 2 * NZ), F32),
            vmem((16, SPAD * 16), F32),
            vmem((16, 384), F32),
            vmem((NPC, LX, 1, NZ), F32),
            vmem((NPC, LX, 1, NZ), F32),
            vmem((NG, CAP, WIDE), F32),
            vmem((NG, CAP, WIDE), F32),
            vmem((2, NPC, LY, NZ), F32),
            vmem((NPC, HID), BF),
            vmem((1, HID), F32),
            vmem((HID, HID), BF),
            vmem((1, HID), F32),
            vmem((NPC, HID), BF),
            vmem((1, PB), jnp.int32),
            vmem((1, PB), jnp.int32),
            vmem((NPC, SPEC), BF),
            pltpu.SMEM((1, NPC), F32),
            vmem((16, HID), F32),
            vmem((8, HID, NZ), BF),
            vmem((HID, NZ), F32),
            vmem((64, HID), BF),
            vmem((16, NZ), F32),
            vmem((48, 4 * NZ), F32),
            dma((12,)),
            dma((SPEC // PART,)),
            dma((NCH,)),
            dma((2,)),
            dma((2,)),
            dma((2,)),
            dma((2,)),
            dma((NG,)),
            dma((NG,)),
        ],
        compiler_params=pltpu.CompilerParams(collective_id=0, has_side_effects=True, vmem_limit_bytes=40 * 1024 * 1024),
        name="section_step",
    )(*[pltpu.with_memory_space_constraint(v, pltpu.HBM) for v in (
        base_scores, section_scores, section_scores.reshape(NPC, LX, LY, 1, NZ), velocity, diffusivity,
        w_first.T, b_first.reshape(1, HID), w_second, b_second.reshape(1, HID), w_third, b_third.reshape(1, NPC),
        loadings, parcel_species.transpose(1, 0, 2), parcel_owner.reshape(1, PB), parcel_block.reshape(1, PB),
    )])


def solution(mesh):
    placed = (
        P(None, "gx", "gy", None), P(None, "gx", "gy", None), P(None, "gx", "gy", None), P("gx", "gy", None),
        P(), P(), P(), P(), P(), P(), P(),
        P(("gx", "gy"), None, None), P(("gx", "gy"), None), P(("gx", "gy")),
    )
    return jax.shard_map(
        shards, mesh=mesh, in_specs=placed, out_specs=P(None, "gx", "gy", None), check_vma=False
    )
```

```python
import jax
import jax.numpy as jnp
from jax import lax
from jax.experimental import pallas as pl
from jax.experimental.pallas import tpu as pltpu
from jax.sharding import PartitionSpec as P

BF = jnp.bfloat16
F32 = jnp.float32
MESH = pl.DeviceIdType.MESH

NPC = 12
SPEC = 300
SPAD = 320
PART = 60
HID = 256
LX, LY, NZ = 32, 16, 128
PB = 32
CAP = 4
SB = 32
NG = 16
CH = 4
NCH = LX // CH
PAIRS = CH // 2
DT = 0.25
WIDE = (NPC + 1) * NZ
CROWS = 144


def iota(shape, dim):
    return lax.broadcasted_iota(jnp.int32, shape, dim)


def kernel(
    base, section, edges, velocity, diffusivity, w1t, b1, w2, b2, w3, b3, loadings, parcels, owner, block,
    result,
    sec, basev, velv, diffv, chem, par, proj, lrep, lpad, ylo, yhi, send, recv, spr,
    w1tv, b1v, w2v, b2v, w3v, ownv, blkv, loadv, b3s, a16, w1s, b2c, w3p, b3c, rest,
    in_sem, par_sem, chunk_sem, xs, xr, ys, yr, ssem, rsem,
):
    gx = lax.axis_index("gx")
    gy = lax.axis_index("gy")

    barrier = pltpu.get_barrier_semaphore()
    for d in range(1, NG):
        pl.semaphore_signal(barrier, inc=1, device_id={"gy": lax.rem(gy + d, NG)}, device_id_type=MESH)

    @pl.when(gx > 0)
    def _():
        pl.semaphore_signal(barrier, inc=1, device_id={"gx": gx - 1}, device_id_type=MESH)

    @pl.when(gx < NG - 1)
    def _():
        pl.semaphore_signal(barrier, inc=1, device_id={"gx": gx + 1}, device_id_type=MESH)

    small = [
        pltpu.make_async_copy(a, b, in_sem.at[i])
        for i, (a, b) in enumerate(
            [(w1t, w1tv), (b1, b1v), (w2, w2v), (b2, b2v), (w3, w3v), (b3, b3s), (loadings, loadv), (owner, ownv), (block, blkv)]
        )
    ]
    for c in small:
        c.start()

    def chunk_copy(c):
        return pltpu.make_async_copy(
            section.at[:, pl.ds(CH * c, CH)], sec.at[:, pl.ds(1 + CH * c, CH), pl.ds(8, LY)], chunk_sem.at[c]
        )

    def parcel_copy(i):
        return pltpu.make_async_copy(parcels.at[pl.ds(PART * i, PART)], par.at[pl.ds(PART * i, PART)], par_sem.at[i])

    chunk_copy(1).start()
    parcel_copy(0).start()
    parcel_copy(1).start()
    chunk_copy(2).start()
    parcel_copy(2).start()
    chunk_copy(3).start()
    parcel_copy(3).start()
    chunk_copy(4).start()
    parcel_copy(4).start()
    for c in (5, 6, 7, 0):
        chunk_copy(c).start()
    big = [
        pltpu.make_async_copy(a, b, in_sem.at[9 + i])
        for i, (a, b) in enumerate([(velocity, velv), (diffusivity, diffv), (base, basev)])
    ]
    for c in big:
        c.start()

    for c in small:
        c.wait()
    par[SPEC:SPAD] = jnp.zeros((SPAD - SPEC, PB, NZ), BF)
    bias = b1v[...]
    hi = bias.astype(BF).astype(F32)
    mid = (bias - hi).astype(BF).astype(F32)
    a16[0:NPC, :] = w1tv[...].astype(F32)
    a16[12:13, :] = hi
    a16[13:14, :] = mid
    a16[14:15, :] = (bias - hi) - mid
    a16[15:16, :] = jnp.zeros((1, HID), F32)
    left = a16[...].T.astype(BF)
    row, lane = iota((16, NZ), 0), iota((16, NZ), 1)
    for j in range(8):
        pick = ((lane < 96) & (lane // 8 == row) & (lane % 8 == j)) | ((lane >= 96) & (lane - 96 + 12 == row) & (row < 15))
        w1s[j] = jnp.dot(left, pick.astype(F32).astype(BF), preferred_element_type=F32).astype(BF)
    b2c[...] = jnp.broadcast_to(b2v[...], (NZ, HID)).T
    w3p[...] = jnp.zeros((48, HID), BF)
    w3p[0:NPC, :] = (w3v[...].astype(F32) * (0.25 * DT)).astype(BF)
    col = jnp.zeros((16, NZ), F32)
    for k in range(NPC):
        col = jnp.where(row == k, b3s[0, k] * (0.25 * DT), col)
    b3c[...] = col
    lpad[...] = jnp.zeros((16, 384), F32)
    lpad[0:NPC, 0:SPEC] = loadv[...].astype(F32)
    for g in range(SPAD // 8):
        tile = lpad[:, (8 * g // 128) * 128 : (8 * g // 128) * 128 + 128]
        lrep[:, 128 * g : 128 * g + 128] = jnp.take_along_axis(tile, (8 * g) % 128 + lane // 16, axis=1)
    diagonal = (iota((16, 256), 1) % 16) == iota((16, 256), 0)

    proj[...] = jnp.zeros((NPC * 16, 2 * NZ), F32)

    def halo_x(up):
        return pltpu.make_async_remote_copy(
            section.at[:, LX - 1 if up else 0], sec.at[:, 0 if up else LX + 1, pl.ds(8, LY)],
            xs.at[0 if up else 1], xr.at[0 if up else 1],
            device_id={"gx": gx + 1 if up else gx - 1}, device_id_type=MESH,
        )

    def halo_y(up):
        return pltpu.make_async_remote_copy(
            edges.at[:, :, LY - 1 if up else 0], ylo if up else yhi,
            ys.at[0 if up else 1], yr.at[0 if up else 1],
            device_id={"gy": gy + 1 if up else gy - 1}, device_id_type=MESH,
        )

    def regress(c, aside):
        n = 8 * PAIRS
        ones = (iota((32, NZ), 0) < 3).astype(F32).astype(BF)
        bias2 = jnp.concatenate([b2c[...]] * 4, axis=1)
        bias3 = jnp.concatenate([b3c[...]] * 4, axis=1)
        cells, first, second = {}, {}, {}
        for t in range(n + 3):
            if t >= 3:
                u = t - 3
                three = jnp.dot(w3p[...], second.pop(u), preferred_element_type=F32)
                rest[...] = three[16:, :]
                three = three[:16, :] + bias3
                for dx in range(2):
                    for o in range(2):
                        h = 2 * dx + o
                        chem[CH * c + 2 * (u // 8) + dx, o, pl.ds(u % 8, 16, stride=9), :] = three[:, NZ * h : NZ * h + NZ]
            if t < n:
                if t % 8 == 0:
                    parts = []
                    for dx in range(2):
                        for o in range(2):
                            v = sec[:, CH * c + 1 + 2 * (t // 8) + dx, 8 + 8 * o : 16 + 8 * o, :]
                            parts.append(jnp.concatenate([v.reshape(96, NZ).astype(BF), ones], axis=0))
                    cells[t // 8] = jnp.concatenate(parts, axis=1)
                one = jnp.dot(w1s[t % 8], cells[t // 8], preferred_element_type=F32)
                first[t] = jnp.tanh(one).astype(BF)
            if 1 <= t <= n:
                two = jnp.dot(w2v[...], first.pop(t - 1), preferred_element_type=F32)
                second[t - 1] = jnp.tanh(two + bias2).astype(BF)
            aside(t)

    lane3 = iota((LY, NZ), 1)

    def combine(x, extra=None):
        e = x + 1
        sec[:, e, 7:8, :] = ylo[:, x]
        sec[:, e, 24:25, :] = yhi[:, x]
        d = diffv[x] * (0.25 * DT)
        vx, vy, vz = (velv[i, x] * (-0.125 * DT) for i in range(3))
        up = jnp.where(lane3 == NZ - 1, 0.0, d + vz)
        down = jnp.where(lane3 == 0, 0.0, d - vz)
        c = sec[:, e, 8:24, :]
        total = 0.75 * basev[:, x] + (0.25 - 6.0 * d) * c
        total += (d + vx) * sec[:, e + 1, 8:24, :] + (d - vx) * sec[:, e - 1, 8:24, :]
        total += (d + vy) * sec[:, e, 9:25, :] + (d - vy) * sec[:, e, 7:23, :]
        total += up * pltpu.roll(c, NZ - 1, axis=2) + down * pltpu.roll(c, 1, axis=2)
        if extra is not None:
            total += spr[extra]
        for k in range(NPC):
            for o in range(2):
                result[k, x, 8 * o : 8 * o + 8, :] = total[k, 8 * o : 8 * o + 8] + chem[x, o, 9 * k : 9 * k + 8, :]

    def project(c):
        left = []
        for k in range(NPC):
            line = lrep[k : k + 1, pl.ds(pl.multiple_of(256 * c, 256), 256)]
            left.append(jnp.where(diagonal, jnp.broadcast_to(line, (16, 256)), 0.0).astype(BF))
        right = [par[pl.ds(16 * c, 16), 16 * h : 16 * h + 16, :].reshape(256, NZ) for h in range(2)]
        right = jnp.concatenate(right, axis=1)
        return jnp.concatenate(
            [jnp.dot(jnp.concatenate(left[i : i + 6], axis=0), right, preferred_element_type=F32) for i in (0, 6)], axis=0
        )

    def open_step(b, carry):
        chunk_copy(b + 1).wait()
        parcel_copy(b + 1).wait()
        got = []

        def aside(t):
            if t == 1:
                for _ in range(5):
                    got.append(project(5 * b + len(got)))

        regress(b + 1, aside)
        proj[...] += sum(got)
        return carry

    parcel_copy(0).wait()
    lax.fori_loop(0, 1, open_step, 0)

    pl.semaphore_wait(barrier, NG - 1 + (gx > 0).astype(jnp.int32) + (gx < NG - 1).astype(jnp.int32))

    pl.when(gy < NG - 1)(lambda: halo_y(True).start())
    pl.when(gy > 0)(lambda: halo_y(False).start())
    pl.when(gx < NG - 1)(lambda: halo_x(True).start())
    pl.when(gx > 0)(lambda: halo_x(False).start())

    lax.fori_loop(1, NCH // 2, open_step, 0)

    projected = proj[...].astype(BF)
    eye = iota((PB, PB), 0) == iota((PB, PB), 1)
    own_row = jnp.broadcast_to(ownv[...].astype(F32), (PB, PB))
    own_col = jnp.sum(jnp.where(eye, own_row, 0.0), axis=1, keepdims=True)
    earlier = (own_row == own_col) & (iota((PB, PB), 0) < iota((PB, PB), 1))
    rank = jnp.sum(jnp.where(earlier, 1.0, 0.0), axis=0, keepdims=True)
    slot = jnp.broadcast_to(ownv[...].astype(F32) * CAP + rank, (NG * CAP, PB))
    chosen = (slot == iota((NG * CAP, PB), 0).astype(F32)).astype(F32).astype(BF)
    blk_row = jnp.broadcast_to(blkv[...].astype(F32) + 1.0, (PB, PB))
    tag = jnp.broadcast_to(jnp.sum(jnp.where(eye, blk_row, 0.0), axis=1, keepdims=True), (PB, NZ)).astype(BF)
    pieces = [
        jnp.concatenate([projected[16 * k : 16 * k + 16, 0:NZ], projected[16 * k : 16 * k + 16, NZ : 2 * NZ]], axis=0)
        for k in range(NPC)
    ]
    values = jnp.dot(chosen, jnp.concatenate(pieces + [tag], axis=1), preferred_element_type=F32)
    for i in range(NG):
        send[i] = values[CAP * i : CAP * i + CAP, :]
    recv[gy] = send[gy]

    def exchange(d):
        peer = lax.rem(gy + d, NG)
        return pltpu.make_async_remote_copy(
            send.at[peer], recv.at[gy], ssem.at[d], rsem.at[d], device_id={"gy": peer}, device_id_type=MESH
        )

    for d in range(1, NG):
        exchange(d).start()

    @pl.when(gx > 0)
    def _():
        halo_x(True).wait_recv()

    @pl.when(gx == 0)
    def _():
        sec[:, 0, 8:24, :] = jnp.zeros((NPC, LY, NZ), F32)

    @pl.when(gx < NG - 1)
    def _():
        halo_x(False).wait_recv()

    @pl.when(gx == NG - 1)
    def _():
        sec[:, LX + 1, 8:24, :] = jnp.zeros((NPC, LY, NZ), F32)

    @pl.when(gy > 0)
    def _():
        halo_y(True).wait_recv()

    @pl.when(gy == 0)
    def _():
        ylo[...] = jnp.zeros((NPC, LX, 1, NZ), F32)

    @pl.when(gy < NG - 1)
    def _():
        halo_y(False).wait_recv()

    @pl.when(gy == NG - 1)
    def _():
        yhi[...] = jnp.zeros((NPC, LX, 1, NZ), F32)

    for c in (5, 6, 7, 0):
        chunk_copy(c).wait()
    for c in big:
        c.wait()

    def step(b, carry):
        late, early = 2 * b - NCH + 1, jnp.maximum(2 * b - NCH, 1)

        def aside(t):
            if t % 2 == 1 and t // 2 < 2 * CH:
                i = t // 2
                combine(CH * (early if i < CH else late) + i % CH)

        chunk = lax.rem(b + 1, NCH)
        regress(chunk, aside)
        return carry

    lax.fori_loop(NCH // 2, NCH, step, 0)
    for d in range(1, NG):
        exchange(d).wait_recv()
    got = jnp.concatenate([recv[i] for i in range(NG)], axis=0)
    place = (got[:, NPC * NZ :] - 1.0 == iota((NG * CAP, NZ), 1).astype(F32)).astype(F32).T[0:SB].astype(BF)
    mine = jnp.dot(place, got[:, 0 : NPC * NZ].astype(BF), preferred_element_type=F32) * (0.25 * DT)
    for k in range(NPC):
        for x in range(2):
            spr[x, k] = mine[LY * x : LY * x + LY, NZ * k : NZ * k + NZ]
    for x in range(CH):
        combine(x, x if x < 2 else None)
    for d in range(1, NG):
        exchange(d).wait_send()
    pl.when(gy < NG - 1)(lambda: halo_y(True).wait_send())
    pl.when(gy > 0)(lambda: halo_y(False).wait_send())
    pl.when(gx < NG - 1)(lambda: halo_x(True).wait_send())
    pl.when(gx > 0)(lambda: halo_x(False).wait_send())


def shards(
    base_scores, section_scores, velocity, diffusivity, w_first, b_first, w_second, b_second, w_third, b_third,
    loadings, parcel_species, parcel_owner, parcel_block,
):
    anywhere = pl.BlockSpec(memory_space=pltpu.HBM)
    vmem = pltpu.VMEM
    dma = pltpu.SemaphoreType.DMA
    return pl.pallas_call(
        kernel,
        out_shape=jax.ShapeDtypeStruct((NPC, LX, LY, NZ), F32),
        in_specs=[anywhere] * 15,
        out_specs=pl.BlockSpec(memory_space=pltpu.VMEM),
        scratch_shapes=[
            vmem((NPC, LX + 2, 2 * LY, NZ), F32),
            vmem((NPC, LX, LY, NZ), F32),
            vmem((3, LX, LY, NZ), F32),
            vmem((LX, LY, NZ), F32),
            vmem((LX, 2, CROWS, NZ), F32),
            vmem((SPAD, PB, NZ), BF),
            vmem((NPC * 16, 2 * NZ), F32),
            vmem((16, SPAD * 16), F32),
            vmem((16, 384), F32),
            vmem((NPC, LX, 1, NZ), F32),
            vmem((NPC, LX, 1, NZ), F32),
            vmem((NG, CAP, WIDE), F32),
            vmem((NG, CAP, WIDE), F32),
            vmem((2, NPC, LY, NZ), F32),
            vmem((NPC, HID), BF),
            vmem((1, HID), F32),
            vmem((HID, HID), BF),
            vmem((1, HID), F32),
            vmem((NPC, HID), BF),
            vmem((1, PB), jnp.int32),
            vmem((1, PB), jnp.int32),
            vmem((NPC, SPEC), BF),
            pltpu.SMEM((1, NPC), F32),
            vmem((16, HID), F32),
            vmem((8, HID, NZ), BF),
            vmem((HID, NZ), F32),
            vmem((48, HID), BF),
            vmem((16, NZ), F32),
            vmem((32, 4 * NZ), F32),
            dma((12,)),
            dma((SPEC // PART,)),
            dma((NCH,)),
            dma((2,)),
            dma((2,)),
            dma((2,)),
            dma((2,)),
            dma((NG,)),
            dma((NG,)),
        ],
        compiler_params=pltpu.CompilerParams(collective_id=0, has_side_effects=True, vmem_limit_bytes=40 * 1024 * 1024),
        name="section_step",
    )(*[pltpu.with_memory_space_constraint(v, pltpu.HBM) for v in (
        base_scores, section_scores, section_scores.reshape(NPC, LX, LY, 1, NZ), velocity, diffusivity,
        w_first.T, b_first.reshape(1, HID), w_second, b_second.reshape(1, HID), w_third, b_third.reshape(1, NPC),
        loadings, parcel_species.transpose(1, 0, 2), parcel_owner.reshape(1, PB), parcel_block.reshape(1, PB),
    )])


def solution(mesh):
    placed = (
        P(None, "gx", "gy", None), P(None, "gx", "gy", None), P(None, "gx", "gy", None), P("gx", "gy", None),
        P(), P(), P(), P(), P(), P(), P(),
        P(("gx", "gy"), None, None), P(("gx", "gy"), None), P(("gx", "gy")),
    )
    return jax.shard_map(
        shards, mesh=mesh, in_specs=placed, out_specs=P(None, "gx", "gy", None), check_vma=False
    )
```
